128 devices in a mesh: lat: 32 (over x, y, core), lon: 4 (over z).
Axes of the slice: x: 4, y: 4, z: 4, core: 2. Of those that a mesh axis runs over, the one named last changes fastest.
Arguments:
- coeffs_old: float32 [640, 2, 3, 50, 640], P(('lat', 'lon')), may hold values from -0.16 to 0.16
- noise: bfloat16 [640, 2, 3, 50, 640], P(('lat', 'lon')), may hold values from -6 to 6
- legendre: float32 [640, 640, 640], P(('lat', 'lon')), may hold values from -0.25 to 0.25
- decay: float32 [3], replicated, may hold values from 0.3 to 0.97
- amplitude: float32 [3, 640], replicated, may hold values from 0.005 to 0.05
- wavenumber_of_slot: int32 [640], replicated, may hold values from 0 to 639, as said below
- lat_order: int32 [640], replicated, may hold values from 0 to 639, each once
Outputs:
- coeffs_new: float32 [640, 2, 3, 50, 640], P(('lat', 'lon'))
- pattern: float32 [640, 50, 1280], P(('lat', 'lon'))
The draws below stay inside these ranges and needn't reach their ends.
Inputs may be any that keep to these rules, and one draw needn't show every extreme that they name: `wavenumber_of_slot`: every wavenumber fills exactly one slot; the sums of the wavenumbers of one device's 5 slots differ between devices by less than 128. `lat_order`: every latitude stands in exactly one row.
All inputs are finite; a program needn't handle non-finite values.
Results may differ from the reference program's by a relative error of at most 0.0003.
Values sent between devices are 32-bit elements; how exact they have to be, the bound alone decides.
No kernel may reach another device: no remote copies, remote signals or barrier semaphores. Data moves between devices by JAX's collectives and lax.ppermute only.
A program may use at most 128 MiB of HBM per device.

```python
import math
import jax
import jax.numpy as jnp
from jax import lax

M = 640
LAT = 640
LON = 1280
SCALES = 3
MEMBERS = 50
SLOT_DEV = 5


def draw_wavenumber_of_slot(key, part):
    devices_all = M // SLOT_DEV
    position = jax.random.permutation(jax.random.fold_in(key, 11), devices_all).astype(jnp.int32)
    rounds = jnp.arange(SLOT_DEV, dtype=jnp.int32)
    dealt = jnp.where(rounds[None, :] % 2 == 0, position[:, None], devices_all - 1 - position[:, None])
    table = rounds[None, :] * devices_all + dealt
    return table.reshape(-1).astype(jnp.int32)


def shard_levels(stream_key, shape, cuts, low, high):
    def one(dim, blocks):
        steps = jax.random.uniform(jax.random.fold_in(jax.random.fold_in(stream_key, 6), dim), (blocks,), jnp.float32, low / len(cuts), high / len(cuts))
        return jnp.repeat(jnp.exp(steps), shape[dim] // blocks).reshape((-1,) + (1,) * (len(shape) - dim - 1))

    loudness = one(*cuts[0])
    for cut in cuts[1:]:
        loudness = loudness * one(*cut)
    return loudness


def scatter_about(own_key, dims, scale, bound, shards=(), kind=jnp.bfloat16):
    result = scale * jax.random.normal(own_key, dims, jnp.float32)
    if shards:
        result = result * shard_levels(own_key, dims, shards, -0.22, 0.18)
    return jnp.clip(result, -bound, bound).astype(kind)


def setup_inputs(seed: int = 0) -> dict:
    arg_keys = jax.random.split(jax.random.key(seed), 8)
    coeffs_old = scatter_about(arg_keys[0], (M, 2, SCALES, MEMBERS, M), 0.02, 0.16, ((0, 128),), jnp.float32)
    noise = scatter_about(arg_keys[1], (M, 2, SCALES, MEMBERS, M), 1.0, 6.0, ((0, 128),))
    legendre = scatter_about(arg_keys[2], (M, LAT, M), M ** -0.5, 0.25, ((0, 128),), jnp.float32)
    decay = jnp.clip(jax.random.uniform(arg_keys[3], (SCALES,), jnp.float32, 0.3, 0.97), 0.3, 0.97)
    amplitude = jnp.clip(jnp.exp(jax.random.uniform(arg_keys[4], (SCALES, M), jnp.float32, math.log(0.005), math.log(0.05))), 0.005, 0.05)
    wavenumber_of_slot = draw_wavenumber_of_slot(jax.random.fold_in(arg_keys[7], 71), 0)
    lat_order = jax.random.permutation(arg_keys[6], LAT).astype(jnp.int32)
    return {"coeffs_old": coeffs_old, "noise": noise, "legendre": legendre, "decay": decay, "amplitude": amplitude, "wavenumber_of_slot": wavenumber_of_slot, "lat_order": lat_order}


def evolve(coeffs_old, noise, decay, amplitude, waves):
    width = coeffs_old.shape[4]
    offsets = lax.broadcasted_iota(jnp.int32, (waves.shape[0], width), 1)
    live = waves[:, None] + offsets < width
    padded = jnp.concatenate([amplitude, jnp.zeros_like(amplitude)], axis=1)
    spread = jax.vmap(lambda wave: lax.dynamic_slice_in_dim(padded, wave, width, 1))(waves)
    factor = jnp.sqrt(1.0 - decay * decay)
    fresh = decay[None, None, :, None, None] * coeffs_old + (spread * factor[None, :, None])[:, None, :, None, :] * noise.astype(jnp.float32)
    return jnp.where(live[:, None, None, None, :], fresh, jnp.zeros_like(fresh))

def reference(coeffs_old, noise, legendre, decay, amplitude, wavenumber_of_slot, lat_order):
    waves = wavenumber_of_slot.astype(jnp.int32)
    coeffs_new = evolve(coeffs_old, noise, decay, amplitude, waves)

    def per_slot(pair):
        coeff, basis = pair
        return jnp.einsum('rkej,lj->rel', coeff, basis, precision=lax.Precision.HIGHEST)
    field = lax.map(per_slot, (coeffs_new, legendre))
    real_part = jnp.zeros((M,) + field.shape[2:], field.dtype).at[waves].set(field[:, 0])
    imag_part = jnp.zeros((M,) + field.shape[2:], field.dtype).at[waves].set(field[:, 1])
    positive = jnp.arange(M, dtype=jnp.int32)[:, None, None] > 0
    imag_part = jnp.where(positive, imag_part, jnp.zeros_like(imag_part))
    real_part = jnp.take(real_part, lat_order.astype(jnp.int32), axis=2)
    imag_part = jnp.take(imag_part, lat_order.astype(jnp.int32), axis=2)
    spectrum = real_part + 1j * imag_part
    grid = jnp.fft.irfft(spectrum, n=LON, axis=0) * LON
    pattern = jnp.transpose(grid, (2, 1, 0))
    return (coeffs_new, pattern)
```

```python
import functools

import jax
import jax.numpy as jnp
from jax import lax
from jax.experimental import pallas as pl
from jax.experimental.pallas import tpu as pltpu
from jax.sharding import PartitionSpec as P

LON = 1280
TWO_PI = 6.283185307179586
AXES = ("lat", "lon")
F32 = jnp.float32
BF16 = jnp.bfloat16
LANES = 128


def split(x):
    high = x.astype(BF16)
    return high, (x - high.astype(F32)).astype(BF16)


def slot_factors(amp_ref, decay_ref, wave):
    scales, width = amp_ref.shape
    row = lax.broadcasted_iota(jnp.int32, (scales, width), 0)
    lane = lax.broadcasted_iota(jnp.int32, (scales, width), 1)
    decay = jnp.full((scales, width), decay_ref[0], F32)
    for k in range(1, scales):
        decay = jnp.where(row == k, decay_ref[k], decay)
    rolled = pltpu.roll(amp_ref[...], lax.rem(width - wave, width), 1)
    live = lane + wave < width
    zero = jnp.zeros((scales, width), F32)
    return (
        jnp.where(live, decay, zero),
        jnp.where(live, rolled * jnp.sqrt(1.0 - decay * decay), zero),
    )


def first_slot(slots):
    return (lax.axis_index("lat") * lax.axis_size("lon") + lax.axis_index("lon")) * slots


def field_kernel(
    waves_h, order_h, decay_h, amp_h, old_h, noise_h, leg_h, send_ref,
    waves, order, decay_ref, amp_ref, old_v, noise_v, leg_v, w_ref, f_ref, fac_ref, sems, small_sems,
):
    slots, scales, members, parts, width = old_h.shape
    lats = leg_h.shape[1]
    pairs = members * parts
    base = first_slot(slots)
    lane_tiles = f_ref.shape[0] // lats

    def copies(s, jt):
        cols = pl.ds(pl.multiple_of(jt * LANES, LANES), LANES)
        return (
            pltpu.make_async_copy(old_h.at[s, :, :, :, cols], old_v.at[s, :, :, :, cols], sems.at[s, jt, 0]),
            pltpu.make_async_copy(noise_h.at[s, :, :, :, cols], noise_v.at[s, :, :, :, cols], sems.at[s, jt, 1]),
            pltpu.make_async_copy(leg_h.at[s, :, cols], leg_v.at[s, :, cols], sems.at[s, jt, 2]),
        )

    small = [
        pltpu.make_async_copy(src, dst, small_sems.at[i])
        for i, (src, dst) in enumerate(
            ((waves_h, waves), (decay_h, decay_ref), (amp_h, amp_ref), (order_h, order))
        )
    ]
    for c in small:
        c.start()
    for s in range(slots):
        for c in copies(s, 0):
            c.start()
    f_ref[...] = jnp.zeros_like(f_ref)
    w_ref[...] = jnp.zeros_like(w_ref)
    for c in small[:3]:
        c.wait()
    counts = [(width - waves[base + s] + LANES - 1) // LANES for s in range(slots)]
    for s in range(slots):

        def start(jt, _, s=s):
            for c in copies(s, jt):
                c.start()
            return 0

        lax.fori_loop(1, counts[s], start, 0)
    for s in range(slots):
        decay, noise_factor = slot_factors(amp_ref, decay_ref, waves[base + s])
        fac_ref[s, 0] = decay
        fac_ref[s, 1] = noise_factor
    contract = (((1,), (1,)), ((), ()))
    for s in range(slots):
        tile, offset = divmod(s * pairs, LANES)
        wide = 2 if offset + pairs > LANES else 1

        def step(jt, _, s=s, tile=tile, offset=offset, wide=wide):
            cols = pl.ds(pl.multiple_of(jt * LANES, LANES), LANES)
            for c in copies(s, jt):
                c.wait()
            d = fac_ref[s, 0, :, cols]
            a = fac_ref[s, 1, :, cols]
            total = None
            for k in range(scales):
                term = d[k].reshape(1, 1, LANES) * old_v[s, k, :, :, cols] + a[k].reshape(1, 1, LANES) * noise_v[
                    s, k, :, :, cols
                ].astype(F32)
                total = term if total is None else total + term
            w_ref[s, offset : offset + pairs, :] = total.reshape(pairs, LANES)
            wh, wl = split(w_ref[s, : wide * LANES, :])
            lh, ll = split(leg_v[s, :, cols])
            res = lax.dot_general(
                jnp.concatenate([lh, ll], axis=1), jnp.concatenate([wh, wh], axis=1), contract,
                preferred_element_type=F32,
            ) + lax.dot_general(lh, wl, contract, preferred_element_type=F32)
            for w in range(wide):
                rows = pl.ds(tile + w, lats, stride=lane_tiles)
                f_ref[rows, :] = f_ref[rows, :] + res[:, w * LANES : (w + 1) * LANES]
            return 0

        lax.fori_loop(0, counts[s], step, 0)

    small[3].wait()
    f3 = f_ref.reshape(lats, lane_tiles, LANES)
    unroll = 8

    def gather(i, _):
        for u in range(unroll):
            q = i * unroll + u
            send_ref[q] = f3[order[q]]
        return 0

    lax.fori_loop(0, lats // unroll, gather, 0)


def evolve_kernel(waves, decay_ref, amp_ref, old_ref, noise_ref, new_ref, *, slots):
    scales = amp_ref.shape[0]
    d, a = slot_factors(amp_ref, decay_ref, waves[first_slot(slots) + pl.program_id(0)])
    for k in range(scales):
        new_ref[0, k] = d[k : k + 1][None] * old_ref[0, k] + a[k : k + 1][None] * noise_ref[0, k].astype(F32)


def trig(steps):
    turns = jnp.floor((steps + 0.5) * (1.0 / LON))
    rest = steps - turns * LON
    quarter = jnp.floor((rest + LON / 8) * (4.0 / LON))
    x = (rest - quarter * (LON / 4)) * (TWO_PI / LON)
    y = x * x
    sine = x * (1.0 + y * (-1.0 / 6 + y * (1.0 / 120 + y * (-1.0 / 5040 + y * (1.0 / 362880)))))
    cosine = 1.0 + y * (-0.5 + y * (1.0 / 24 + y * (-1.0 / 720 + y * (1.0 / 40320 - y * (1.0 / 3628800)))))
    odd = (quarter == 1.0) | (quarter == 3.0)
    c = jnp.where(odd, sine, cosine)
    s = jnp.where(odd, cosine, sine)
    c = jnp.where((quarter == 1.0) | (quarter == 2.0), -c, c)
    s = jnp.where((quarter == 2.0) | (quarter == 3.0), -s, s)
    return c, s


def table_kernel(wave_ref, high_ref, low_ref):
    count, slots = wave_ref.shape
    length = high_ref.shape[1]
    lane = lax.broadcasted_iota(jnp.int32, (count, LANES), 1)
    for s in range(slots):
        wave = jnp.broadcast_to(wave_ref[:, s : s + 1], (count, LANES))
        weight = jnp.where(wave == 0, 1.0, 2.0).astype(F32)
        c, n = trig((wave * lane).astype(F32))
        c1, n1 = trig((wave * LANES).astype(F32))
        c = c * weight
        n = -n * weight
        for b in range(length // LANES):
            cols = slice(b * LANES, (b + 1) * LANES)
            for r, value in enumerate((c, n)):
                rows = slice((2 * s + r) * count, (2 * s + r + 1) * count)
                high, low = split(value)
                high_ref[rows, cols] = high
                low_ref[rows, cols] = low
            c, n = c * c1 + n * n1, n * c1 - c * n1


def synthesis_kernel(recv_ref, high_ref, low_ref, out_ref, t_ref, x_ref, xx_ref, *, sources, slots):
    rows, members, block = out_ref.shape
    pitch = -(-members // 8) * 8
    tall = rows * pitch
    second = -(-tall // 16) * 16
    pairs = members * 2
    lane_tiles = recv_ref.shape[0] // (sources * rows)

    @pl.when(pl.program_id(0) == 0)
    def _():
        for q in range(rows):
            for t in range(lane_tiles):
                piece = recv_ref[pl.ds(q * lane_tiles + t, sources, stride=rows * lane_tiles), :]
                t_ref[q, t * LANES : (t + 1) * LANES, :] = piece.T
            for s in range(slots):
                for r in range(2):
                    g = 2 * s + r
                    x_ref[q * pitch : (q + 1) * pitch, g * sources : (g + 1) * sources] = t_ref[
                        q, pl.ds(s * pairs + r, pitch, stride=2), :
                    ]
        high, low = split(x_ref[...])
        xx_ref[0:tall, :] = high
        xx_ref[second : second + tall, :] = low

    both = jnp.dot(xx_ref[...], high_ref[...], preferred_element_type=F32)
    res = both[0:tall] + both[second : second + tall] + jnp.dot(
        xx_ref[0:tall, :], low_ref[...], preferred_element_type=F32
    )
    for q in range(rows):
        out_ref[q] = res[q * pitch : q * pitch + members]


def in_hbm(x):
    return pltpu.with_memory_space_constraint(x, pltpu.HBM)


def local(coeffs_old, noise, legendre, decay, amplitude, wavenumber_of_slot, lat_order):
    devices = lax.axis_size(AXES)
    slots, parts, scales, members, width = coeffs_old.shape
    lats = legendre.shape[1]
    rows = lats // devices
    waves = wavenumber_of_slot.astype(jnp.int32)
    order = lat_order.astype(jnp.int32)
    old = coeffs_old.transpose(0, 2, 3, 1, 4)
    fresh = noise.transpose(0, 2, 3, 1, 4)
    lane_tiles = -(-slots * parts * members // LANES)
    smem = pl.BlockSpec(memory_space=pltpu.SMEM)
    vmem = pl.BlockSpec(memory_space=pltpu.VMEM)
    hbm = pl.BlockSpec(memory_space=pltpu.HBM)

    with jax.named_scope("field"):
        send = pl.pallas_call(
            field_kernel,
            in_specs=[hbm] * 7,
            out_specs=vmem,
            out_shape=jax.ShapeDtypeStruct((lats, lane_tiles, LANES), F32),
            scratch_shapes=[
                pltpu.SMEM(waves.shape, jnp.int32),
                pltpu.SMEM(order.shape, jnp.int32),
                pltpu.SMEM(decay.shape, F32),
                pltpu.VMEM(amplitude.shape, F32),
                pltpu.VMEM((slots, scales, members, parts, width), F32),
                pltpu.VMEM((slots, scales, members, parts, width), BF16),
                pltpu.VMEM((slots, lats, width), F32),
                pltpu.VMEM((slots, 2 * LANES, LANES), F32),
                pltpu.VMEM((lats * lane_tiles, LANES), F32),
                pltpu.VMEM((slots, 2, scales, width), F32),
                pltpu.SemaphoreType.DMA((slots, width // LANES, 3)),
                pltpu.SemaphoreType.DMA((4,)),
            ],
            compiler_params=pltpu.CompilerParams(vmem_limit_bytes=40 << 20),
            cost_estimate=pl.CostEstimate(flops=10**9, transcendentals=0, bytes_accessed=14 * 10**6),
        )(*[in_hbm(x) for x in (waves, order, decay, amplitude, old, fresh, legendre)])

    with jax.named_scope("exchange"):
        recv = lax.all_to_all(send, AXES, split_axis=0, concat_axis=0, tiled=True)

    with jax.named_scope("evolve"):
        block = (1, scales, members, parts, width)
        new = pl.pallas_call(
            functools.partial(evolve_kernel, slots=slots),
            grid=(slots,),
            in_specs=[smem, smem, vmem] + [pl.BlockSpec(block, lambda i: (i, 0, 0, 0, 0))] * 2,
            out_specs=pl.BlockSpec(block, lambda i: (i, 0, 0, 0, 0)),
            out_shape=jax.ShapeDtypeStruct(old.shape, F32),
            compiler_params=pltpu.CompilerParams(vmem_limit_bytes=16 << 20),
            cost_estimate=pl.CostEstimate(flops=5 * 10**8, transcendentals=0, bytes_accessed=10**7),
        )(waves, decay, amplitude, old, fresh)
    coeffs_new = new.transpose(0, 3, 1, 2, 4)

    with jax.named_scope("table"):
        terms = devices * slots * parts
        high, low = pl.pallas_call(
            table_kernel,
            out_shape=[jax.ShapeDtypeStruct((terms, LON), BF16)] * 2,
            compiler_params=pltpu.CompilerParams(vmem_limit_bytes=24 << 20),
            cost_estimate=pl.CostEstimate(flops=5 * 10**8, transcendentals=0, bytes_accessed=7 * 10**6),
        )(waves.reshape(devices, slots))

    with jax.named_scope("synthesis"):
        cut = 256
        pitch = -(-members // 8) * 8
        tall = rows * pitch
        second = -(-tall // 16) * 16
        pattern = pl.pallas_call(
            functools.partial(synthesis_kernel, sources=devices, slots=slots),
            grid=(LON // cut,),
            in_specs=[vmem] + [pl.BlockSpec((terms, cut), lambda i: (0, i), memory_space=pltpu.VMEM)] * 2,
            out_specs=pl.BlockSpec((rows, members, cut), lambda i: (0, 0, i)),
            out_shape=jax.ShapeDtypeStruct((rows, members, LON), F32),
            scratch_shapes=[
                pltpu.VMEM((rows, lane_tiles * LANES, devices), F32),
                pltpu.VMEM((tall, terms), F32),
                pltpu.VMEM((2 * second, terms), BF16),
            ],
            compiler_params=pltpu.CompilerParams(vmem_limit_bytes=32 << 20),
        )(recv.reshape(lats * lane_tiles, LANES), in_hbm(high), in_hbm(low))
    return (coeffs_new, pattern)


def solution(mesh):
    split_first = P(AXES, None, None, None, None)
    in_specs = (split_first, split_first, P(AXES, None, None), P(), P(), P(), P())
    out_specs = (split_first, P(AXES, None, None))
    return jax.shard_map(local, mesh=mesh, in_specs=in_specs, out_specs=out_specs, check_vma=False)
```

```python
import functools

import jax
import jax.numpy as jnp
from jax import lax
from jax.experimental import pallas as pl
from jax.experimental.pallas import tpu as pltpu
from jax.sharding import PartitionSpec as P

LON = 1280
TWO_PI = 6.283185307179586
AXES = ("lat", "lon")
F32 = jnp.float32
BF16 = jnp.bfloat16
LANES = 128


def split(x):
    high = x.astype(BF16)
    return high, (x - high.astype(F32)).astype(BF16)


def slot_factors(amp_ref, decay_ref, wave):
    scales, width = amp_ref.shape
    row = lax.broadcasted_iota(jnp.int32, (scales, width), 0)
    lane = lax.broadcasted_iota(jnp.int32, (scales, width), 1)
    decay = jnp.full((scales, width), decay_ref[0], F32)
    for k in range(1, scales):
        decay = jnp.where(row == k, decay_ref[k], decay)
    rolled = pltpu.roll(amp_ref[...], lax.rem(width - wave, width), 1)
    live = lane + wave < width
    zero = jnp.zeros((scales, width), F32)
    return (
        jnp.where(live, decay, zero),
        jnp.where(live, rolled * jnp.sqrt(1.0 - decay * decay), zero),
    )


def first_slot(slots):
    return (lax.axis_index("lat") * lax.axis_size("lon") + lax.axis_index("lon")) * slots


def field_kernel(
    waves_h, order_h, decay_h, amp_h, old_h, noise_h, leg_h, send_h,
    waves, order, decay_ref, amp_ref, old_v, noise_v, leg_v, w_ref, f_ref, fac_ref, list_ref, send_v,
    sems, small_sems, out_sems,
):
    slots, scales, members, parts, width = old_h.shape
    lats = leg_h.shape[1]
    pairs = members * parts
    base = first_slot(slots)
    lane_tiles = send_h.shape[1]
    tiles = width // LANES
    ring = sems.shape[0]
    old_p = old_v.reshape(old_v.shape[0], old_v.shape[1] // parts, parts, LANES)

    def place(i):
        s = list_ref[i] // tiles
        jt = lax.rem(list_ref[i], tiles)
        return s, jt, pl.ds(pl.multiple_of(jt * LANES, LANES), LANES)

    def copies(i):
        s, jt, cols = place(i)
        here = pl.ds((s * tiles + jt) * scales, scales)
        slot = lax.rem(i, ring)
        return (
            pltpu.make_async_copy(old_h.at[s, :, :, :, cols], old_p.at[here, 0:members], sems.at[slot, 0]),
            pltpu.make_async_copy(noise_h.at[s, :, :, :, cols], noise_v.at[here], sems.at[slot, 1]),
            pltpu.make_async_copy(leg_h.at[s, :, cols], leg_v.at[s, jt], sems.at[slot, 2]),
        )

    def begin(i):
        for c in copies(i):
            c.start()

    def arrive(i):
        for c in copies(i):
            c.wait()

    small = [
        pltpu.make_async_copy(src, dst, small_sems.at[i])
        for i, (src, dst) in enumerate(
            ((waves_h, waves), (decay_h, decay_ref), (amp_h, amp_ref), (order_h, order))
        )
    ]
    for c in small:
        c.start()
    for s in range(slots):
        list_ref[s] = s * tiles
    for i in range(min(ring, slots)):
        begin(i)
    f_ref[...] = jnp.zeros_like(f_ref)
    w_ref[...] = jnp.zeros_like(w_ref)
    for c in small[:3]:
        c.wait()
    live = slots
    for s in range(slots):
        count = (width - waves[base + s] + LANES - 1) // LANES

        def note(jt, live, s=s):
            list_ref[live] = s * tiles + jt
            return live + 1

        live = lax.fori_loop(1, count, note, live)
    for s in range(slots):
        decay, noise_factor = slot_factors(amp_ref, decay_ref, waves[base + s])
        fac_ref[s, 0] = decay
        fac_ref[s, 1] = noise_factor
    contract = (((1,), (1,)), ((), ()))

    group = 10

    def coefficients(i, buffer):
        s, jt, cols = place(i)
        d = fac_ref[s, 0, :, cols]
        a = fac_ref[s, 1, :, cols]
        at = (s * tiles + jt) * scales
        offset = lax.rem(s * pairs, LANES)
        for g in range(0, members, group):
            fresh = None
            for k in range(scales):
                term = a[k].reshape(1, 1, LANES) * noise_v[at + k, g : g + group].astype(F32)
                fresh = term if fresh is None else fresh + term
            total = fresh.reshape(group * parts, LANES)
            for k in range(scales):
                total = total + d[k : k + 1] * old_v[at + k, g * parts : (g + group) * parts]
            w_ref[buffer, s, pl.ds(offset + g * parts, group * parts), :] = total

    def product(i, buffer, scale):
        s, jt, cols = place(i)
        spread = w_ref.at[buffer, s]
        w = (spread[0:LANES, :] + spread[LANES : 2 * LANES, :]) * scale
        w = jnp.concatenate(split(w), axis=0)
        leg = jnp.concatenate(split(leg_v[s, jt]), axis=1)
        res = lax.dot_general(leg, jnp.concatenate([w, w], axis=1), contract, preferred_element_type=F32)
        rows = pl.ds(s, lats, stride=slots)
        f_ref[rows, :] = f_ref[rows, :] + (res[:, :LANES] + res[:, LANES:])

    unroll = 1
    last = live - 1
    for u in range(unroll):
        arrive(u)
        coefficients(u, u)

    def step(n, _):
        first = n * unroll
        for u in range(unroll):
            ahead = first + u + ring

            @pl.when((ahead >= min(ring, slots)) & (ahead < live))
            def _(ahead=ahead):
                begin(ahead)

        for u in range(unroll):
            coming = first + unroll + u

            @pl.when(coming < live)
            def _(coming=coming):
                arrive(coming)

        here = lax.rem(n, 2) * unroll
        there = unroll - here
        for u in range(unroll):
            i = first + u
            product(jnp.minimum(i, last), here + u, jnp.where(i < live, 1.0, 0.0).astype(F32))
        for u in range(unroll):
            coefficients(jnp.minimum(first + unroll + u, last), there + u)
        return 0

    lax.fori_loop(0, (live + unroll - 1) // unroll, step, 0)
    small[3].wait()
    row = lax.broadcasted_iota(jnp.int32, (lane_tiles, LANES), 0)
    lane = lax.broadcasted_iota(jnp.int32, (lane_tiles, LANES), 1)
    lower = row * LANES + lane < (row + 1) * pairs
    many = 32
    pieces = out_sems.shape[0]
    part = lats // pieces
    out = []
    for p in range(pieces):

        def gather(i, _, p=p):
            for u in range(many):
                q = p * part + i * many + u
                at = order[q] * slots
                send_v[q] = jnp.where(lower, f_ref[pl.ds(at, lane_tiles), :], f_ref[pl.ds(at + 1, lane_tiles), :])
            return 0

        lax.fori_loop(0, part // many, gather, 0)
        rows = pl.ds(p * part, part)
        out.append(pltpu.make_async_copy(send_v.at[rows], send_h.at[rows], out_sems.at[p]))
        out[-1].start()
    for c in out:
        c.wait()


def evolve_kernel(waves, decay_ref, amp_ref, old_ref, noise_ref, new_ref, *, slots):
    scales = amp_ref.shape[0]
    d, a = slot_factors(amp_ref, decay_ref, waves[first_slot(slots) + pl.program_id(0)])
    for k in range(scales):
        new_ref[0, k] = d[k : k + 1][None] * old_ref[0, k] + a[k : k + 1][None] * noise_ref[0, k].astype(F32)


def trig(steps):
    turns = jnp.floor((steps + 0.5) * (1.0 / LON))
    rest = steps - turns * LON
    quarter = jnp.floor((rest + LON / 8) * (4.0 / LON))
    x = (rest - quarter * (LON / 4)) * (TWO_PI / LON)
    y = x * x
    sine = x * (1.0 + y * (-1.0 / 6 + y * (1.0 / 120 + y * (-1.0 / 5040 + y * (1.0 / 362880)))))
    cosine = 1.0 + y * (-0.5 + y * (1.0 / 24 + y * (-1.0 / 720 + y * (1.0 / 40320))))
    odd = (quarter == 1.0) | (quarter == 3.0)
    c = jnp.where(odd, sine, cosine)
    s = jnp.where(odd, cosine, sine)
    c = jnp.where((quarter == 1.0) | (quarter == 2.0), -c, c)
    s = jnp.where((quarter == 2.0) | (quarter == 3.0), -s, s)
    return c, s


def synthesis_kernel(
    recv_ref, wave_ref, out_h, c_ref, n_ref, c1_ref, n1_ref, high_v, low_v, out_v, t_ref, x_ref, xx_ref, out_sems,
):
    sources, slots = wave_ref.shape
    blocks, terms, block = high_v.shape
    rows, members, _ = out_h.shape
    pitch = -(-members // 8) * 8
    tall = rows * pitch
    second = -(-tall // 16) * 16
    pairs = members * 2
    lane_tiles = recv_ref.shape[0] // (sources * rows)
    lane = lax.broadcasted_iota(jnp.int32, (sources, LANES), 1)
    leap_c, leap_s = trig((wave_ref[...] * LANES).astype(F32))
    for s in range(slots):
        wave = jnp.broadcast_to(wave_ref[:, s : s + 1], (sources, LANES))
        weight = jnp.where(wave == 0, 1.0, 2.0).astype(F32)
        c, n = trig((wave * lane).astype(F32))
        c_ref[s] = c * weight
        n_ref[s] = -n * weight
        c1_ref[s] = jnp.broadcast_to(leap_c[:, s : s + 1], (sources, LANES))
        n1_ref[s] = jnp.broadcast_to(leap_s[:, s : s + 1], (sources, LANES))
    for q in range(rows):
        for t in range(lane_tiles):
            piece = recv_ref[pl.ds(q * lane_tiles + t, sources, stride=rows * lane_tiles), :]
            t_ref[q, t * LANES : (t + 1) * LANES, :] = piece.T
        for s in range(slots):
            for r in range(2):
                g = 2 * s + r
                x_ref[q * pitch : (q + 1) * pitch, g * sources : (g + 1) * sources] = t_ref[
                    q, pl.ds(s * pairs + r, pitch, stride=2), :
                ]
    high, low = split(x_ref[...])
    xx_ref[0:tall, :] = high
    xx_ref[second : second + tall, :] = low

    def table(b):
        for s in range(slots):
            c, n, c1, n1 = c_ref[s], n_ref[s], c1_ref[s], n1_ref[s]
            for p in range(block // LANES):
                cols = slice(p * LANES, (p + 1) * LANES)
                for r, value in enumerate((c, n)):
                    at = slice((2 * s + r) * sources, (2 * s + r + 1) * sources)
                    high, low = split(value)
                    high_v[b, at, cols] = high
                    low_v[b, at, cols] = low
                c, n = c * c1 + n * n1, n * c1 - c * n1
            c_ref[s] = c
            n_ref[s] = n

    table(0)
    stores = []
    for b in range(blocks):
        both = jnp.dot(xx_ref[...], high_v[b], preferred_element_type=F32)
        res = both[0:tall] + both[second : second + tall] + jnp.dot(
            xx_ref[0:tall, :], low_v[b], preferred_element_type=F32
        )
        if b + 1 < blocks:
            table(b + 1)
        cols = pl.ds(b * block, block)
        for q in range(rows):
            out_v[q, :, cols] = res[q * pitch : q * pitch + members]
        store = pltpu.make_async_copy(out_v.at[:, :, cols], out_h.at[:, :, cols], out_sems.at[b])
        store.start()
        stores.append(store)
    for c in stores:
        c.wait()


def in_hbm(x):
    return pltpu.with_memory_space_constraint(x, pltpu.HBM)


def spec(space):
    return pl.BlockSpec(memory_space=space)


def run_field(waves, order, decay, amplitude, old, noise, legendre):
    slots, scales, members, parts, width = old.shape
    lats = legendre.shape[1]
    lane_tiles = -(-slots * parts * members // LANES)
    pitch = -(-parts * members // 16) * 16
    return pl.pallas_call(
        field_kernel,
        in_specs=[spec(pltpu.HBM)] * 7,
        out_specs=spec(pltpu.HBM),
        out_shape=pltpu.HBM((lats, lane_tiles, LANES), F32),
        scratch_shapes=[
            pltpu.SMEM(waves.shape, jnp.int32),
            pltpu.SMEM(order.shape, jnp.int32),
            pltpu.SMEM(decay.shape, F32),
            pltpu.VMEM(amplitude.shape, F32),
            pltpu.VMEM((slots * (width // LANES) * scales, pitch, LANES), F32),
            pltpu.VMEM((slots * (width // LANES) * scales, members, parts, LANES), BF16),
            pltpu.VMEM((slots, width // LANES, lats, LANES), F32),
            pltpu.VMEM((2 * 1, slots, 2 * LANES, LANES), F32),
            pltpu.VMEM((lats * slots, LANES), F32),
            pltpu.VMEM((slots, 2, scales, width), F32),
            pltpu.SMEM((slots * width // LANES,), jnp.int32),
            pltpu.VMEM((lats, lane_tiles, LANES), F32),
            pltpu.SemaphoreType.DMA((4, 3)),
            pltpu.SemaphoreType.DMA((4,)),
            pltpu.SemaphoreType.DMA((4,)),
        ],
        compiler_params=pltpu.CompilerParams(vmem_limit_bytes=40 << 20),
        cost_estimate=pl.CostEstimate(flops=10**9, transcendentals=0, bytes_accessed=14 * 10**6),
    )(*[in_hbm(x) for x in (waves, order, decay, amplitude, old, noise, legendre)])


def run_evolve(waves, decay, amplitude, old, noise):
    slots = old.shape[0]
    block = pl.BlockSpec((1,) + old.shape[1:], lambda i: (i, 0, 0, 0, 0))
    return pl.pallas_call(
        functools.partial(evolve_kernel, slots=slots),
        grid=(slots,),
        in_specs=[spec(pltpu.SMEM), spec(pltpu.SMEM), spec(pltpu.VMEM), block, block],
        out_specs=block,
        out_shape=jax.ShapeDtypeStruct(old.shape, F32),
        compiler_params=pltpu.CompilerParams(vmem_limit_bytes=16 << 20),
        cost_estimate=pl.CostEstimate(flops=5 * 10**8, transcendentals=0, bytes_accessed=10**7),
    )(waves, decay, amplitude, old, noise)


def run_synthesis(recv, wave_table, rows, members):
    sources, slots = wave_table.shape
    cut = 256
    blocks = LON // cut
    terms = sources * slots * 2
    tall = rows * (-(-members // 8) * 8)
    second = -(-tall // 16) * 16
    lane_tiles = recv.shape[0] // (sources * rows)
    return pl.pallas_call(
        synthesis_kernel,
        in_specs=[spec(pltpu.VMEM)] * 2,
        out_specs=spec(pltpu.HBM),
        out_shape=pltpu.HBM((rows, members, LON), F32),
        scratch_shapes=[pltpu.VMEM((slots, sources, LANES), F32)] * 4
        + [
            pltpu.VMEM((blocks, terms, cut), BF16),
            pltpu.VMEM((blocks, terms, cut), BF16),
            pltpu.VMEM((rows, members, LON), F32),
            pltpu.VMEM((rows, lane_tiles * LANES, sources), F32),
            pltpu.VMEM((tall, terms), F32),
            pltpu.VMEM((2 * second, terms), BF16),
            pltpu.SemaphoreType.DMA((blocks,)),
        ],
        compiler_params=pltpu.CompilerParams(vmem_limit_bytes=32 << 20),
    )(recv, wave_table)


def local(coeffs_old, noise, legendre, decay, amplitude, wavenumber_of_slot, lat_order):
    devices = lax.axis_size(AXES)
    slots, parts, scales, members, width = coeffs_old.shape
    lats = legendre.shape[1]
    waves = wavenumber_of_slot.astype(jnp.int32)
    order = lat_order.astype(jnp.int32)
    old = coeffs_old.transpose(0, 2, 3, 1, 4)
    fresh = noise.transpose(0, 2, 3, 1, 4)
    with jax.named_scope("field"):
        send = run_field(waves, order, decay, amplitude, old, fresh, legendre)
    with jax.named_scope("exchange"):
        recv = lax.all_to_all(send, AXES, split_axis=0, concat_axis=0, tiled=True)
    with jax.named_scope("evolve"):
        new = run_evolve(waves, decay, amplitude, old, fresh)
    with jax.named_scope("synthesis"):
        pattern = run_synthesis(recv.reshape(-1, LANES), waves.reshape(devices, slots), lats // devices, members)
    return (new.transpose(0, 3, 1, 2, 4), pattern)


def solution(mesh):
    split_first = P(AXES, None, None, None, None)
    in_specs = (split_first, split_first, P(AXES, None, None), P(), P(), P(), P())
    out_specs = (split_first, P(AXES, None, None))
    return jax.shard_map(local, mesh=mesh, in_specs=in_specs, out_specs=out_specs, check_vma=False)
```

```python
import functools

import jax
import jax.numpy as jnp
from jax import lax
from jax.experimental import pallas as pl
from jax.experimental.pallas import tpu as pltpu
from jax.sharding import PartitionSpec as P

LON = 1280
TWO_PI = 6.283185307179586
AXES = ("lat", "lon")
F32 = jnp.float32
BF16 = jnp.bfloat16
LANES = 128


def split(x):
    high = x.astype(BF16)
    return high, (x - high.astype(F32)).astype(BF16)


def slot_factors(amp_ref, decay_ref, wave):
    scales, width = amp_ref.shape
    row = lax.broadcasted_iota(jnp.int32, (scales, width), 0)
    lane = lax.broadcasted_iota(jnp.int32, (scales, width), 1)
    decay = jnp.full((scales, width), decay_ref[0], F32)
    for k in range(1, scales):
        decay = jnp.where(row == k, decay_ref[k], decay)
    rolled = pltpu.roll(amp_ref[...], lax.rem(width - wave, width), 1)
    live = lane + wave < width
    zero = jnp.zeros((scales, width), F32)
    return (
        jnp.where(live, decay, zero),
        jnp.where(live, rolled * jnp.sqrt(1.0 - decay * decay), zero),
    )


def first_slot(slots):
    return (lax.axis_index("lat") * lax.axis_size("lon") + lax.axis_index("lon")) * slots


def field_kernel(
    waves_h, order_h, decay_h, amp_h, old_h, noise_h, leg_h, send_h,
    waves, order, decay_ref, amp_ref, old_v, noise_v, leg_v, w_ref, f_ref, fac_ref, list_ref, send_v,
    sems, small_sems, out_sems,
):
    slots, scales, members, parts, width = old_h.shape
    lats = leg_h.shape[1]
    pairs = members * parts
    base = first_slot(slots)
    lane_tiles = send_h.shape[1]
    tiles = width // LANES
    ring = sems.shape[0]
    old_p = old_v.reshape(old_v.shape[0], old_v.shape[1] // parts, parts, LANES)

    def place(i):
        s = list_ref[0, i]
        jt = list_ref[1, i]
        return s, jt, pl.ds(pl.multiple_of(jt * LANES, LANES), LANES)

    def copies(i):
        s, jt, cols = place(i)
        here = pl.ds((s * tiles + jt) * scales, scales)
        slot = lax.rem(i, ring)
        return (
            pltpu.make_async_copy(old_h.at[s, :, :, :, cols], old_p.at[here, 0:members], sems.at[slot, 0]),
            pltpu.make_async_copy(noise_h.at[s, :, :, :, cols], noise_v.at[here], sems.at[slot, 1]),
            pltpu.make_async_copy(leg_h.at[s, :, cols], leg_v.at[s, jt], sems.at[slot, 2]),
        )

    def begin(i):
        for c in copies(i):
            c.start()

    def arrive(i):
        for c in copies(i):
            c.wait()

    small = [
        pltpu.make_async_copy(src, dst, small_sems.at[i])
        for i, (src, dst) in enumerate(
            ((waves_h, waves), (decay_h, decay_ref), (amp_h, amp_ref), (order_h, order))
        )
    ]
    for c in small:
        c.start()
    for s in range(slots):
        list_ref[0, s] = s
        list_ref[1, s] = 0
    for i in range(min(ring, slots)):
        begin(i)
    f_ref[...] = jnp.zeros_like(f_ref)
    w_ref[...] = jnp.zeros_like(w_ref)
    for c in small[:3]:
        c.wait()
    live = slots
    for s in range(slots):
        count = (width - waves[base + s] + LANES - 1) // LANES

        def note(jt, live, s=s):
            list_ref[0, live] = s
            list_ref[1, live] = jt
            return live + 1

        live = lax.fori_loop(1, count, note, live)
    for s in range(slots):
        decay, noise_factor = slot_factors(amp_ref, decay_ref, waves[base + s])
        fac_ref[s, 0] = decay
        fac_ref[s, 1] = noise_factor
    contract = (((1,), (1,)), ((), ()))

    group = 10

    def coefficients(i, buffer):
        s, jt, cols = place(i)
        d = fac_ref[s, 0, :, cols]
        a = fac_ref[s, 1, :, cols]
        at = (s * tiles + jt) * scales
        offset = lax.rem(s * pairs, LANES)
        target = w_ref.at[buffer, s]
        for g in range(0, members, group):
            fresh = None
            for k in range(scales):
                term = a[k].reshape(1, 1, LANES) * noise_v[at + k, g : g + group].astype(F32)
                fresh = term if fresh is None else fresh + term
            for e in range(group):
                target[pl.ds(offset + (g + e) * parts, parts), :] = fresh[e]
        rows = pl.ds(offset, pairs)
        total = target[rows, :]
        for k in range(scales):
            total = total + d[k : k + 1] * old_v[at + k, 0:pairs]
        target[rows, :] = total

    def product(i, buffer, scale):
        s, jt, cols = place(i)
        spread = w_ref.at[buffer, s]
        w = (spread[0:LANES, :] + spread[LANES : 2 * LANES, :]) * scale
        w = jnp.concatenate(split(w), axis=0)
        leg = jnp.concatenate(split(leg_v[s, jt]), axis=1)
        res = lax.dot_general(leg, jnp.concatenate([w, w], axis=1), contract, preferred_element_type=F32)
        rows = pl.ds(s, lats, stride=slots)
        f_ref[rows, :] = f_ref[rows, :] + (res[:, :LANES] + res[:, LANES:])

    unroll = 1
    last = live - 1
    for u in range(unroll):
        arrive(u)
        coefficients(u, u)

    def step(n, _):
        first = n * unroll
        for u in range(unroll):
            ahead = first + u + ring

            @pl.when((ahead >= min(ring, slots)) & (ahead < live))
            def _(ahead=ahead):
                begin(ahead)

        for u in range(unroll):
            coming = first + unroll + u

            @pl.when(coming < live)
            def _(coming=coming):
                arrive(coming)

        here = lax.rem(n, 2) * unroll
        there = unroll - here
        for u in range(unroll):
            i = first + u
            product(jnp.minimum(i, last), here + u, jnp.where(i < live, 1.0, 0.0).astype(F32))
        for u in range(unroll):
            coefficients(jnp.minimum(first + unroll + u, last), there + u)
        return 0

    lax.fori_loop(0, (live + unroll - 1) // unroll, step, 0)
    small[3].wait()
    row = lax.broadcasted_iota(jnp.int32, (lane_tiles, LANES), 0)
    lane = lax.broadcasted_iota(jnp.int32, (lane_tiles, LANES), 1)
    lower = row * LANES + lane < (row + 1) * pairs
    many = 32
    pieces = out_sems.shape[0]
    part = lats // pieces
    out = []
    for p in range(pieces):

        def gather(i, _, p=p):
            for u in range(many):
                q = p * part + i * many + u
                at = order[q] * slots
                send_v[q] = jnp.where(lower, f_ref[pl.ds(at, lane_tiles), :], f_ref[pl.ds(at + 1, lane_tiles), :])
            return 0

        lax.fori_loop(0, part // many, gather, 0)
        rows = pl.ds(p * part, part)
        out.append(pltpu.make_async_copy(send_v.at[rows], send_h.at[rows], out_sems.at[p]))
        out[-1].start()
    for c in out:
        c.wait()


def evolve_kernel(waves, decay_ref, amp_ref, old_ref, noise_ref, new_ref, *, slots):
    scales = amp_ref.shape[0]
    d, a = slot_factors(amp_ref, decay_ref, waves[first_slot(slots) + pl.program_id(0)])
    for k in range(scales):
        new_ref[0, k] = d[k : k + 1][None] * old_ref[0, k] + a[k : k + 1][None] * noise_ref[0, k].astype(F32)


def trig(steps):
    turns = jnp.floor((steps + 0.5) * (1.0 / LON))
    rest = steps - turns * LON
    quarter = jnp.floor((rest + LON / 8) * (4.0 / LON))
    x = (rest - quarter * (LON / 4)) * (TWO_PI / LON)
    y = x * x
    sine = x * (1.0 + y * (-1.0 / 6 + y * (1.0 / 120 + y * (-1.0 / 5040 + y * (1.0 / 362880)))))
    cosine = 1.0 + y * (-0.5 + y * (1.0 / 24 + y * (-1.0 / 720 + y * (1.0 / 40320))))
    odd = (quarter == 1.0) | (quarter == 3.0)
    c = jnp.where(odd, sine, cosine)
    s = jnp.where(odd, cosine, sine)
    c = jnp.where((quarter == 1.0) | (quarter == 2.0), -c, c)
    s = jnp.where((quarter == 2.0) | (quarter == 3.0), -s, s)
    return c, s


def synthesis_kernel(
    recv_ref, wave_ref, out_h, c_ref, n_ref, c1_ref, n1_ref, high_v, low_v, out_v, t_ref, x_ref, xx_ref, g_ref, out_sems,
):
    sources, slots = wave_ref.shape
    blocks, kinds, _, block = high_v.shape
    rows, members, length = out_h.shape
    pitch = -(-members // 8) * 8
    tall = rows * pitch
    second = -(-tall // 16) * 16
    pairs = members * 2
    half = length // 2
    tiles = half // LANES
    lane_tiles = recv_ref.shape[0] // (sources * rows)
    lane = lax.broadcasted_iota(jnp.int32, (sources, LANES), 1)
    leap_c, leap_s = trig((wave_ref[...] * LANES).astype(F32))
    for s in range(slots):
        wave = jnp.broadcast_to(wave_ref[:, s : s + 1], (sources, LANES))
        weight = jnp.where(wave == 0, 1.0, 2.0).astype(F32)
        c, n = trig((wave * lane).astype(F32))
        c_ref[s] = c * weight
        n_ref[s] = -n * weight
        c1_ref[s] = jnp.broadcast_to(leap_c[:, s : s + 1], (sources, LANES))
        n1_ref[s] = jnp.broadcast_to(leap_s[:, s : s + 1], (sources, LANES))
    for q in range(rows):
        for t in range(lane_tiles):
            piece = recv_ref[pl.ds(q * lane_tiles + t, sources, stride=rows * lane_tiles), :]
            t_ref[q, t * LANES : (t + 1) * LANES, :] = piece.T
        for s in range(slots):
            for r in range(kinds):
                x_ref[r, q * pitch : (q + 1) * pitch, s * sources : (s + 1) * sources] = t_ref[
                    q, pl.ds(s * pairs + r, pitch, stride=2), :
                ]
    for r in range(kinds):
        high, low = split(x_ref[r])
        xx_ref[r, 0:tall, :] = high
        xx_ref[r, second : second + tall, :] = low

    def table(b):
        for s in range(slots):
            c, n, c1, n1 = c_ref[s], n_ref[s], c1_ref[s], n1_ref[s]
            for p in range(block // LANES):
                cols = slice(p * LANES, (p + 1) * LANES)
                for r, value in enumerate((c, n)):
                    at = slice(s * sources, (s + 1) * sources)
                    high, low = split(value)
                    high_v[b, r, at, cols] = high
                    low_v[b, r, at, cols] = low
                c, n = c * c1 + n * n1, n * c1 - c * n1
            c_ref[s] = c
            n_ref[s] = n

    def summed(b, r):
        both = jnp.dot(xx_ref[r], high_v[b, r], preferred_element_type=F32)
        return both[0:tall] + both[second : second + tall] + jnp.dot(
            xx_ref[r, 0:tall, :], low_v[b, r], preferred_element_type=F32
        )

    def leave(first, size, index):
        cols = pl.ds(first, size)
        return pltpu.make_async_copy(out_v.at[:, :, cols], out_h.at[:, :, cols], out_sems.at[index])

    table(0)
    column = lax.broadcasted_iota(jnp.int32, (tall, LANES), 1)
    mirror = lax.rem(LANES - column, LANES)
    stores = []
    for b in range(blocks):
        even = summed(b, 0)
        odd = summed(b, 1)
        if b + 1 < blocks:
            table(b + 1)
        width = min(block, half - b * block)
        forward = even + odd
        for q in range(rows):
            out_v[q, :, b * block : b * block + width] = forward[q * pitch : q * pitch + members, :width]
        g_ref[:, b * block : (b + 1) * block] = even - odd
        stores.append(leave(b * block, width, len(stores)))
        stores[-1].start()
        lowest = b * (block // LANES) - 1
        done = [t for t in range(lowest, lowest + block // LANES) if 0 <= t < tiles]
        for t in done:
            back = jnp.take_along_axis(g_ref[:, t * LANES : (t + 1) * LANES], mirror, axis=1)
            back = jnp.where(column == 0, g_ref[:, (t + 1) * LANES : (t + 2) * LANES], back)
            at = length - (t + 1) * LANES
            for q in range(rows):
                out_v[q, :, at : at + LANES] = back[q * pitch : q * pitch + members]
        stores.append(leave(length - (done[-1] + 1) * LANES, len(done) * LANES, len(stores)))
        stores[-1].start()
    for c in stores:
        c.wait()


def in_hbm(x):
    return pltpu.with_memory_space_constraint(x, pltpu.HBM)


def spec(space):
    return pl.BlockSpec(memory_space=space)


def run_field(waves, order, decay, amplitude, old, noise, legendre):
    slots, scales, members, parts, width = old.shape
    lats = legendre.shape[1]
    lane_tiles = -(-slots * parts * members // LANES)
    pitch = -(-parts * members // 16) * 16
    return pl.pallas_call(
        field_kernel,
        in_specs=[spec(pltpu.HBM)] * 7,
        out_specs=spec(pltpu.HBM),
        out_shape=pltpu.HBM((lats, lane_tiles, LANES), F32),
        scratch_shapes=[
            pltpu.SMEM(waves.shape, jnp.int32),
            pltpu.SMEM(order.shape, jnp.int32),
            pltpu.SMEM(decay.shape, F32),
            pltpu.VMEM(amplitude.shape, F32),
            pltpu.VMEM((slots * (width // LANES) * scales, pitch, LANES), F32),
            pltpu.VMEM((slots * (width // LANES) * scales, members, parts, LANES), BF16),
            pltpu.VMEM((slots, width // LANES, lats, LANES), F32),
            pltpu.VMEM((2 * 1, slots, 2 * LANES, LANES), F32),
            pltpu.VMEM((lats * slots, LANES), F32),
            pltpu.VMEM((slots, 2, scales, width), F32),
            pltpu.SMEM((2, slots * width // LANES), jnp.int32),
            pltpu.VMEM((lats, lane_tiles, LANES), F32),
            pltpu.SemaphoreType.DMA((4, 3)),
            pltpu.SemaphoreType.DMA((4,)),
            pltpu.SemaphoreType.DMA((4,)),
        ],
        compiler_params=pltpu.CompilerParams(vmem_limit_bytes=40 << 20),
        cost_estimate=pl.CostEstimate(flops=10**9, transcendentals=0, bytes_accessed=14 * 10**6),
    )(*[in_hbm(x) for x in (waves, order, decay, amplitude, old, noise, legendre)])


def run_evolve(waves, decay, amplitude, old, noise):
    slots = old.shape[0]
    block = pl.BlockSpec((1,) + old.shape[1:], lambda i: (i, 0, 0, 0, 0))
    return pl.pallas_call(
        functools.partial(evolve_kernel, slots=slots),
        grid=(slots,),
        in_specs=[spec(pltpu.SMEM), spec(pltpu.SMEM), spec(pltpu.VMEM), block, block],
        out_specs=block,
        out_shape=jax.ShapeDtypeStruct(old.shape, F32),
        compiler_params=pltpu.CompilerParams(vmem_limit_bytes=16 << 20),
        cost_estimate=pl.CostEstimate(flops=5 * 10**8, transcendentals=0, bytes_accessed=10**7),
    )(waves, decay, amplitude, old, noise)


def run_synthesis(recv, wave_table, rows, members):
    sources, slots = wave_table.shape
    cut = 256
    blocks = LON // 2 // cut + 1
    terms = sources * slots
    tall = rows * (-(-members // 8) * 8)
    second = -(-tall // 16) * 16
    lane_tiles = recv.shape[0] // (sources * rows)
    return pl.pallas_call(
        synthesis_kernel,
        in_specs=[spec(pltpu.VMEM)] * 2,
        out_specs=spec(pltpu.HBM),
        out_shape=pltpu.HBM((rows, members, LON), F32),
        scratch_shapes=[pltpu.VMEM((slots, sources, LANES), F32)] * 4
        + [
            pltpu.VMEM((blocks, 2, terms, cut), BF16),
            pltpu.VMEM((blocks, 2, terms, cut), BF16),
            pltpu.VMEM((rows, members, LON), F32),
            pltpu.VMEM((rows, lane_tiles * LANES, sources), F32),
            pltpu.VMEM((2, tall, terms), F32),
            pltpu.VMEM((2, 2 * second, terms), BF16),
            pltpu.VMEM((tall, blocks * cut), F32),
            pltpu.SemaphoreType.DMA((2 * blocks,)),
        ],
        compiler_params=pltpu.CompilerParams(vmem_limit_bytes=32 << 20),
    )(recv, wave_table)


def local(coeffs_old, noise, legendre, decay, amplitude, wavenumber_of_slot, lat_order):
    devices = lax.axis_size(AXES)
    slots, parts, scales, members, width = coeffs_old.shape
    lats = legendre.shape[1]
    waves = wavenumber_of_slot.astype(jnp.int32)
    order = lat_order.astype(jnp.int32)
    old = coeffs_old.transpose(0, 2, 3, 1, 4)
    fresh = noise.transpose(0, 2, 3, 1, 4)
    with jax.named_scope("field"):
        send = run_field(waves, order, decay, amplitude, old, fresh, legendre)
    with jax.named_scope("exchange"):
        recv = lax.all_to_all(send, AXES, split_axis=0, concat_axis=0, tiled=True)
    with jax.named_scope("evolve"):
        new = run_evolve(waves, decay, amplitude, old, fresh)
    with jax.named_scope("synthesis"):
        pattern = run_synthesis(recv.reshape(-1, LANES), waves.reshape(devices, slots), lats // devices, members)
    return (new.transpose(0, 3, 1, 2, 4), pattern)


def solution(mesh):
    split_first = P(AXES, None, None, None, None)
    in_specs = (split_first, split_first, P(AXES, None, None), P(), P(), P(), P())
    out_specs = (split_first, P(AXES, None, None))
    return jax.shard_map(local, mesh=mesh, in_specs=in_specs, out_specs=out_specs, check_vma=False)
```

```python
import functools

import jax
import jax.numpy as jnp
from jax import lax
from jax.experimental import pallas as pl
from jax.experimental.pallas import tpu as pltpu
from jax.sharding import PartitionSpec as P

LON = 1280
TWO_PI = 6.283185307179586
AXES = ("lat", "lon")
F32 = jnp.float32
BF16 = jnp.bfloat16
LANES = 128


def split(x):
    high = x.astype(BF16)
    return high, (x - high.astype(F32)).astype(BF16)


def slot_factors(amp_ref, decay_ref, wave):
    scales, width = amp_ref.shape
    row = lax.broadcasted_iota(jnp.int32, (scales, width), 0)
    lane = lax.broadcasted_iota(jnp.int32, (scales, width), 1)
    decay = jnp.full((scales, width), decay_ref[0], F32)
    for k in range(1, scales):
        decay = jnp.where(row == k, decay_ref[k], decay)
    rolled = pltpu.roll(amp_ref[...], lax.rem(width - wave, width), 1)
    live = lane + wave < width
    zero = jnp.zeros((scales, width), F32)
    return (
        jnp.where(live, decay, zero),
        jnp.where(live, rolled * jnp.sqrt(1.0 - decay * decay), zero),
    )


def first_slot(slots):
    return (lax.axis_index("lat") * lax.axis_size("lon") + lax.axis_index("lon")) * slots


def field_kernel(
    waves_h, order_h, decay_h, amp_h, old_h, noise_h, leg_h, send_h,
    waves, order, decay_ref, amp_ref, old_v, noise_v, leg_v, w_ref, f_ref, fac_ref, list_ref, send_v,
    sems, small_sems, out_sems,
):
    slots, scales, members, parts, width = old_h.shape
    lats = leg_h.shape[1]
    pairs = members * parts
    base = first_slot(slots)
    lane_tiles = send_h.shape[1]
    tiles = width // LANES
    ring = sems.shape[0]
    old_p = old_v.reshape(old_v.shape[0], old_v.shape[1] // parts, parts, LANES)

    def place(i):
        s = list_ref[0, i]
        jt = list_ref[1, i]
        return s, jt, pl.ds(pl.multiple_of(jt * LANES, LANES), LANES)

    def copies(i):
        s, jt, cols = place(i)
        here = pl.ds((s * tiles + jt) * scales, scales)
        slot = i & (ring - 1)
        return (
            pltpu.make_async_copy(old_h.at[s, :, :, :, cols], old_p.at[here, 0:members], sems.at[slot, 0]),
            pltpu.make_async_copy(noise_h.at[s, :, :, :, cols], noise_v.at[here], sems.at[slot, 1]),
            pltpu.make_async_copy(leg_h.at[s, :, cols], leg_v.at[s, jt], sems.at[slot, 2]),
        )

    def begin(i):
        for c in copies(i):
            c.start()

    def arrive(i):
        for c in copies(i):
            c.wait()

    small = [
        pltpu.make_async_copy(src, dst, small_sems.at[i])
        for i, (src, dst) in enumerate(
            ((waves_h, waves), (decay_h, decay_ref), (amp_h, amp_ref), (order_h, order))
        )
    ]
    for c in small:
        c.start()
    for s in range(slots):
        list_ref[0, s] = s
        list_ref[1, s] = 0
    for i in range(min(ring, slots)):
        begin(i)
    f_ref[...] = jnp.zeros_like(f_ref)
    w_ref[...] = jnp.zeros_like(w_ref)
    for c in small[:3]:
        c.wait()
    live = slots
    for s in range(slots):
        count = (width - waves[base + s] + LANES - 1) // LANES

        def note(jt, live, s=s):
            list_ref[0, live] = s
            list_ref[1, live] = jt
            return live + 1

        live = lax.fori_loop(1, count, note, live)
    for s in range(slots):
        decay, noise_factor = slot_factors(amp_ref, decay_ref, waves[base + s])
        fac_ref[s, 0] = decay
        fac_ref[s, 1] = noise_factor
    contract = (((1,), (1,)), ((), ()))

    group = 10

    def coefficients(i, buffer):
        s, jt, cols = place(i)
        d = fac_ref[s, 0, :, cols]
        a = fac_ref[s, 1, :, cols]
        at = (s * tiles + jt) * scales
        offset = (s * pairs) & (LANES - 1)
        target = w_ref.at[buffer, s]
        for g in range(0, members, group):
            fresh = None
            for k in range(scales):
                term = a[k].reshape(1, 1, LANES) * noise_v[at + k, g : g + group].astype(F32)
                fresh = term if fresh is None else fresh + term
            for e in range(group):
                target[pl.ds(offset + (g + e) * parts, parts), :] = fresh[e]
        rows = pl.ds(offset, pairs)
        total = target[rows, :]
        for k in range(scales):
            total = total + d[k : k + 1] * old_v[at + k, 0:pairs]
        target[rows, :] = total

    def product(i, buffer, scale):
        s, jt, cols = place(i)
        spread = w_ref.at[buffer, s]
        w = (spread[0:LANES, :] + spread[LANES : 2 * LANES, :]) * scale
        w = jnp.concatenate(split(w), axis=0)
        leg = jnp.concatenate(split(leg_v[s, jt]), axis=1)
        res = lax.dot_general(leg, jnp.concatenate([w, w], axis=1), contract, preferred_element_type=F32)
        rows = pl.ds(s, lats, stride=slots)
        f_ref[rows, :] = f_ref[rows, :] + (res[:, :LANES] + res[:, LANES:])

    unroll = 1
    last = live - 1
    for u in range(unroll):
        arrive(u)
        coefficients(u, u)

    def step(n, _):
        first = n * unroll
        for u in range(unroll):
            ahead = first + u + ring

            @pl.when((ahead >= min(ring, slots)) & (ahead < live))
            def _(ahead=ahead):
                begin(ahead)

        for u in range(unroll):
            coming = first + unroll + u

            @pl.when(coming < live)
            def _(coming=coming):
                arrive(coming)

        here = (n & 1) * unroll
        there = unroll - here
        for u in range(unroll):
            i = first + u
            product(jnp.minimum(i, last), here + u, jnp.where(i < live, 1.0, 0.0).astype(F32))
        for u in range(unroll):
            coefficients(jnp.minimum(first + unroll + u, last), there + u)
        return 0

    lax.fori_loop(0, (live + unroll - 1) // unroll, step, 0)
    small[3].wait()
    row = lax.broadcasted_iota(jnp.int32, (lane_tiles, LANES), 0)
    lane = lax.broadcasted_iota(jnp.int32, (lane_tiles, LANES), 1)
    lower = row * LANES + lane < (row + 1) * pairs
    many = 128
    pieces = out_sems.shape[0]
    part = lats // pieces
    out = []
    for p in range(pieces):

        def gather(i, _, p=p):
            for u in range(many):
                q = p * part + i * many + u
                at = order[q] * slots
                send_v[q] = jnp.where(lower, f_ref[pl.ds(at, lane_tiles), :], f_ref[pl.ds(at + 1, lane_tiles), :])
            return 0

        lax.fori_loop(0, part // many, gather, 0)
        rows = pl.ds(p * part, part)
        out.append(pltpu.make_async_copy(send_v.at[rows], send_h.at[rows], out_sems.at[p]))
        out[-1].start()
    for c in out:
        c.wait()


def evolve_kernel(waves, decay_ref, amp_ref, old_ref, noise_ref, new_ref, *, slots):
    scales = amp_ref.shape[0]
    d, a = slot_factors(amp_ref, decay_ref, waves[first_slot(slots) + pl.program_id(0)])
    for k in range(scales):
        new_ref[0, k] = d[k : k + 1][None] * old_ref[0, k] + a[k : k + 1][None] * noise_ref[0, k].astype(F32)


def trig(steps):
    turns = jnp.floor((steps + 0.5) * (1.0 / LON))
    rest = steps - turns * LON
    quarter = jnp.floor((rest + LON / 8) * (4.0 / LON))
    x = (rest - quarter * (LON / 4)) * (TWO_PI / LON)
    y = x * x
    sine = x * (1.0 + y * (-1.0 / 6 + y * (1.0 / 120 + y * (-1.0 / 5040 + y * (1.0 / 362880)))))
    cosine = 1.0 + y * (-0.5 + y * (1.0 / 24 + y * (-1.0 / 720 + y * (1.0 / 40320))))
    odd = (quarter == 1.0) | (quarter == 3.0)
    c = jnp.where(odd, sine, cosine)
    s = jnp.where(odd, cosine, sine)
    c = jnp.where((quarter == 1.0) | (quarter == 2.0), -c, c)
    s = jnp.where((quarter == 2.0) | (quarter == 3.0), -s, s)
    return c, s


def synthesis_kernel(
    recv_ref, wave_ref, out_h, c_ref, n_ref, c1_ref, n1_ref, high_v, low_v, out_v, t_ref, x_ref, xx_ref, g_ref, out_sems,
):
    sources, slots = wave_ref.shape
    blocks, kinds, _, block = high_v.shape
    rows, members, length = out_h.shape
    pitch = -(-members // 8) * 8
    tall = rows * pitch
    second = -(-tall // 16) * 16
    pairs = members * 2
    half = length // 2
    tiles = half // LANES
    lane_tiles = recv_ref.shape[0] // (sources * rows)
    lane = lax.broadcasted_iota(jnp.int32, (sources, LANES), 1)
    leap_c, leap_s = trig((wave_ref[...] * LANES).astype(F32))
    for s in range(slots):
        wave = jnp.broadcast_to(wave_ref[:, s : s + 1], (sources, LANES))
        weight = jnp.where(wave == 0, 1.0, 2.0).astype(F32)
        c, n = trig((wave * lane).astype(F32))
        c_ref[s] = c * weight
        n_ref[s] = -n * weight
        c1_ref[s] = jnp.broadcast_to(leap_c[:, s : s + 1], (sources, LANES))
        n1_ref[s] = jnp.broadcast_to(leap_s[:, s : s + 1], (sources, LANES))
    for q in range(rows):
        for t in range(lane_tiles):
            piece = recv_ref[pl.ds(q * lane_tiles + t, sources, stride=rows * lane_tiles), :]
            t_ref[q, t * LANES : (t + 1) * LANES, :] = piece.T
        for s in range(slots):
            for r in range(kinds):
                x_ref[r, q * pitch : (q + 1) * pitch, s * sources : (s + 1) * sources] = t_ref[
                    q, pl.ds(s * pairs + r, pitch, stride=2), :
                ]
    for r in range(kinds):
        high, low = split(x_ref[r])
        xx_ref[r, 0:tall, :] = high
        xx_ref[r, second : second + tall, :] = low

    def table(b):
        for s in range(slots):
            c, n, c1, n1 = c_ref[s], n_ref[s], c1_ref[s], n1_ref[s]
            for p in range(block // LANES):
                cols = slice(p * LANES, (p + 1) * LANES)
                for r, value in enumerate((c, n)):
                    at = slice(s * sources, (s + 1) * sources)
                    high, low = split(value)
                    high_v[b, r, at, cols] = high
                    low_v[b, r, at, cols] = low
                c, n = c * c1 + n * n1, n * c1 - c * n1
            c_ref[s] = c
            n_ref[s] = n

    def summed(b, r):
        both = jnp.dot(xx_ref[r], high_v[b, r], preferred_element_type=F32)
        return both[0:tall] + both[second : second + tall] + jnp.dot(
            xx_ref[r, 0:tall, :], low_v[b, r], preferred_element_type=F32
        )

    def leave(first, size, index):
        cols = pl.ds(first, size)
        return pltpu.make_async_copy(out_v.at[:, :, cols], out_h.at[:, :, cols], out_sems.at[index])

    table(0)
    column = lax.broadcasted_iota(jnp.int32, (tall, LANES), 1)
    mirror = lax.rem(LANES - column, LANES)
    stores = []
    for b in range(blocks):
        even = summed(b, 0)
        odd = summed(b, 1)
        if b + 1 < blocks:
            table(b + 1)
        width = min(block, half - b * block)
        forward = even + odd
        for q in range(rows):
            out_v[q, :, b * block : b * block + width] = forward[q * pitch : q * pitch + members, :width]
        g_ref[:, b * block : (b + 1) * block] = even - odd
        stores.append(leave(b * block, width, len(stores)))
        stores[-1].start()
        lowest = b * (block // LANES) - 1
        done = [t for t in range(lowest, lowest + block // LANES) if 0 <= t < tiles]
        for t in done:
            back = jnp.take_along_axis(g_ref[:, t * LANES : (t + 1) * LANES], mirror, axis=1)
            back = jnp.where(column == 0, g_ref[:, (t + 1) * LANES : (t + 2) * LANES], back)
            at = length - (t + 1) * LANES
            for q in range(rows):
                out_v[q, :, at : at + LANES] = back[q * pitch : q * pitch + members]
        stores.append(leave(length - (done[-1] + 1) * LANES, len(done) * LANES, len(stores)))
        stores[-1].start()
    for c in stores:
        c.wait()


def in_hbm(x):
    return pltpu.with_memory_space_constraint(x, pltpu.HBM)


def spec(space):
    return pl.BlockSpec(memory_space=space)


def run_field(waves, order, decay, amplitude, old, noise, legendre):
    slots, scales, members, parts, width = old.shape
    lats = legendre.shape[1]
    lane_tiles = -(-slots * parts * members // LANES)
    pitch = -(-parts * members // 16) * 16
    return pl.pallas_call(
        field_kernel,
        in_specs=[spec(pltpu.HBM)] * 7,
        out_specs=spec(pltpu.HBM),
        out_shape=pltpu.HBM((lats, lane_tiles, LANES), F32),
        scratch_shapes=[
            pltpu.SMEM(waves.shape, jnp.int32),
            pltpu.SMEM(order.shape, jnp.int32),
            pltpu.SMEM(decay.shape, F32),
            pltpu.VMEM(amplitude.shape, F32),
            pltpu.VMEM((slots * (width // LANES) * scales, pitch, LANES), F32),
            pltpu.VMEM((slots * (width // LANES) * scales, members, parts, LANES), BF16),
            pltpu.VMEM((slots, width // LANES, lats, LANES), F32),
            pltpu.VMEM((2 * 1, slots, 2 * LANES, LANES), F32),
            pltpu.VMEM((lats * slots, LANES), F32),
            pltpu.VMEM((slots, 2, scales, width), F32),
            pltpu.SMEM((2, slots * width // LANES), jnp.int32),
            pltpu.VMEM((lats, lane_tiles, LANES), F32),
            pltpu.SemaphoreType.DMA((4, 3)),
            pltpu.SemaphoreType.DMA((4,)),
            pltpu.SemaphoreType.DMA((5,)),
        ],
        compiler_params=pltpu.CompilerParams(vmem_limit_bytes=40 << 20),
        cost_estimate=pl.CostEstimate(flops=10**9, transcendentals=0, bytes_accessed=14 * 10**6),
    )(*[in_hbm(x) for x in (waves, order, decay, amplitude, old, noise, legendre)])


def run_evolve(waves, decay, amplitude, old, noise):
    slots = old.shape[0]
    block = pl.BlockSpec((1,) + old.shape[1:], lambda i: (i, 0, 0, 0, 0))
    return pl.pallas_call(
        functools.partial(evolve_kernel, slots=slots),
        grid=(slots,),
        in_specs=[spec(pltpu.SMEM), spec(pltpu.SMEM), spec(pltpu.VMEM), block, block],
        out_specs=block,
        out_shape=jax.ShapeDtypeStruct(old.shape, F32),
        compiler_params=pltpu.CompilerParams(vmem_limit_bytes=16 << 20),
        cost_estimate=pl.CostEstimate(flops=5 * 10**8, transcendentals=0, bytes_accessed=10**7),
    )(waves, decay, amplitude, old, noise)


def run_synthesis(recv, wave_table, rows, members):
    sources, slots = wave_table.shape
    cut = 256
    blocks = LON // 2 // cut + 1
    terms = sources * slots
    tall = rows * (-(-members // 8) * 8)
    second = -(-tall // 16) * 16
    lane_tiles = recv.shape[0] // (sources * rows)
    return pl.pallas_call(
        synthesis_kernel,
        in_specs=[spec(pltpu.VMEM)] * 2,
        out_specs=spec(pltpu.HBM),
        out_shape=pltpu.HBM((rows, members, LON), F32),
        scratch_shapes=[pltpu.VMEM((slots, sources, LANES), F32)] * 4
        + [
            pltpu.VMEM((blocks, 2, terms, cut), BF16),
            pltpu.VMEM((blocks, 2, terms, cut), BF16),
            pltpu.VMEM((rows, members, LON), F32),
            pltpu.VMEM((rows, lane_tiles * LANES, sources), F32),
            pltpu.VMEM((2, tall, terms), F32),
            pltpu.VMEM((2, 2 * second, terms), BF16),
            pltpu.VMEM((tall, blocks * cut), F32),
            pltpu.SemaphoreType.DMA((2 * blocks,)),
        ],
        compiler_params=pltpu.CompilerParams(vmem_limit_bytes=32 << 20),
    )(recv, wave_table)


def local(coeffs_old, noise, legendre, decay, amplitude, wavenumber_of_slot, lat_order):
    devices = lax.axis_size(AXES)
    slots, parts, scales, members, width = coeffs_old.shape
    lats = legendre.shape[1]
    waves = wavenumber_of_slot.astype(jnp.int32)
    order = lat_order.astype(jnp.int32)
    old = coeffs_old.transpose(0, 2, 3, 1, 4)
    fresh = noise.transpose(0, 2, 3, 1, 4)
    with jax.named_scope("field"):
        send = run_field(waves, order, decay, amplitude, old, fresh, legendre)
    with jax.named_scope("exchange"):
        recv = lax.all_to_all(send, AXES, split_axis=0, concat_axis=0, tiled=True)
    with jax.named_scope("evolve"):
        new = run_evolve(waves, decay, amplitude, old, fresh)
    with jax.named_scope("synthesis"):
        pattern = run_synthesis(recv.reshape(-1, LANES), waves.reshape(devices, slots), lats // devices, members)
    return (new.transpose(0, 3, 1, 2, 4), pattern)


def solution(mesh):
    split_first = P(AXES, None, None, None, None)
    in_specs = (split_first, split_first, P(AXES, None, None), P(), P(), P(), P())
    out_specs = (split_first, P(AXES, None, None))
    return jax.shard_map(local, mesh=mesh, in_specs=in_specs, out_specs=out_specs, check_vma=False)
```
